32 devices in a mesh: fsdp: 16 (over z, y, x), dp: 2 (over core).
Axes of the slice: x: 2, y: 2, z: 4, core: 2. Of those that a mesh axis runs over, the one named last changes fastest.
Arguments:
- tokens: bfloat16 [32, 1024, 768], P(('fsdp', 'dp')), may hold values from -6 to 6
- lengths: int32 [32], P(('fsdp', 'dp')), may hold values from 512 to 1024, as said below
- first_gain: bfloat16 [768], P('fsdp'), may hold values from 0.099609375 to 1.8984375
- first_bias: bfloat16 [768], P('fsdp'), may hold values from -3 to 3
- qkv_weight: bfloat16 [768, 2304], P('fsdp'), may hold values from -0.21875 to 0.21875
- qkv_bias: bfloat16 [2304], P('fsdp'), may hold values from -3 to 3
- out_weight: bfloat16 [768, 768], P('fsdp'), may hold values from -6 to 6
- out_bias: bfloat16 [768], P('fsdp'), may hold values from -3 to 3
- second_gain: bfloat16 [768], P('fsdp'), may hold values from 0.099609375 to 1.8984375
- second_bias: bfloat16 [768], P('fsdp'), may hold values from -3 to 3
- up_weight: bfloat16 [768, 3072], P('fsdp'), may hold values from -0.21875 to 0.21875
- up_bias: bfloat16 [3072], P('fsdp'), may hold values from -3 to 3
- down_weight: bfloat16 [3072, 768], P('fsdp'), may hold values from -0.109375 to 0.109375
- down_bias: bfloat16 [768], P('fsdp'), may hold values from -3 to 3
- cotangent: bfloat16 [32, 1024, 768], P(('fsdp', 'dp')), may hold values from -6 to 6
Outputs:
- block_output: bfloat16 [32, 1024, 768], P(('fsdp', 'dp'))
- input_grad: bfloat16 [32, 1024, 768], P(('fsdp', 'dp'))
- first_gain_grad: float32 [768], P('fsdp')
- first_bias_grad: float32 [768], P('fsdp')
- qkv_weight_grad: float32 [768, 2304], P('fsdp')
- qkv_bias_grad: float32 [2304], P('fsdp')
- out_weight_grad: float32 [768, 768], P('fsdp')
- out_bias_grad: float32 [768], P('fsdp')
- second_gain_grad: float32 [768], P('fsdp')
- second_bias_grad: float32 [768], P('fsdp')
- up_weight_grad: float32 [768, 3072], P('fsdp')
- up_bias_grad: float32 [3072], P('fsdp')
- down_weight_grad: float32 [3072, 768], P('fsdp')
- down_bias_grad: float32 [768], P('fsdp')
The draws below stay inside these ranges and needn't reach their ends.
Inputs may be any that keep to these rules, and one draw needn't show every extreme that they name: `lengths`: each sequence holds 1024 or 512 codons; the first holds 1024.
All inputs are finite; a program needn't handle non-finite values.
Results may differ from the reference program's by a relative error of at most 0.012.
The reference program's roundings to bfloat16 on the way count: a program that leaves them out, or rounds other values in their place, can miss the bound.
Values may be sent and summed in bfloat16 or wider, within the bound.
A program may use at most 256 MiB of HBM per device.

```python
import jax
import jax.numpy as jnp
from jax import lax

D = 768
HEADS = 12
FF = 3072
LEN = 1024
SEQS = 32


def draw_lengths(key, part):
    picks = jax.random.randint(jax.random.fold_in(key, 7), (SEQS,), 0, 11)
    sizes = jnp.where(picks < 3, LEN // 2, LEN).astype(jnp.int32)
    return sizes.at[0].set(LEN)


def steps_of(key, dims, cuts, smallest, high):
    gain = 1.0
    for position, parts in cuts:
        steps = jax.random.uniform(jax.random.fold_in(jax.random.fold_in(key, 6), position), (parts,), jnp.float32, smallest / len(cuts), high / len(cuts))
        gain = gain * jnp.repeat(jnp.exp(steps), dims[position] // parts).reshape((-1,) + (1,) * (len(dims) - 1 - position))
    return gain


def noise(rng, shape, spread, most, split=(), kind=jnp.bfloat16):
    gain = steps_of(rng, shape, split, -0.22, 0.18) if split else 1.0
    values = jax.random.normal(rng, shape, jnp.float32) * spread * gain
    return jnp.minimum(jnp.maximum(values, -most), most).astype(kind)


def setup_inputs(seed: int = 0) -> dict:
    streams_of = jax.random.split(jax.random.key(seed), 16)
    tokens = noise(streams_of[0], (SEQS, LEN, D), 1.0, 6.0, ((0, 32),))
    lengths = draw_lengths(jax.random.fold_in(streams_of[15], 71), 0)
    first_gain = jnp.clip(1.0 + 0.18 * jax.random.normal(streams_of[2], (D,), jnp.float32), 0.099609375, 1.8984375).astype(jnp.bfloat16)
    first_bias = noise(streams_of[3], (D,), 0.5, 3.0, ((0, 16),))
    qkv_weight = noise(streams_of[4], (D, 3 * D), D ** -0.5, 0.21875, ((0, 16),))
    qkv_bias = noise(streams_of[5], (3 * D,), 0.5, 3.0, ((0, 16),))
    out_weight = noise(streams_of[6], (D, D), 1.0, 6.0, ((0, 16),))
    out_bias = noise(streams_of[7], (D,), 0.5, 3.0, ((0, 16),))
    second_gain = jnp.clip(1.0 + 0.18 * jax.random.normal(streams_of[8], (D,), jnp.float32), 0.099609375, 1.8984375).astype(jnp.bfloat16)
    second_bias = noise(streams_of[9], (D,), 0.5, 3.0, ((0, 16),))
    up_weight = noise(streams_of[10], (D, FF), D ** -0.5, 0.21875, ((0, 16),))
    up_bias = noise(streams_of[11], (FF,), 0.5, 3.0, ((0, 16),))
    down_weight = noise(streams_of[12], (FF, D), FF ** -0.5, 0.109375, ((0, 16),))
    down_bias = noise(streams_of[13], (D,), 0.5, 3.0, ((0, 16),))
    cotangent = noise(streams_of[14], (SEQS, LEN, D), 1.0, 6.0, ((0, 32),))
    return {"tokens": tokens, "lengths": lengths, "first_gain": first_gain, "first_bias": first_bias, "qkv_weight": qkv_weight, "qkv_bias": qkv_bias, "out_weight": out_weight, "out_bias": out_bias, "second_gain": second_gain, "second_bias": second_bias, "up_weight": up_weight, "up_bias": up_bias, "down_weight": down_weight, "down_bias": down_bias, "cotangent": cotangent}


@jax.custom_vjp
def low(v):
    return lax.optimization_barrier(v.astype(jnp.bfloat16)).astype(jnp.float32)

@jax.custom_vjp
def low_back(v):
    return v

def low_keep(v):
    return (low(v), None)

def low_pass(kept, grad):
    return (grad,)

def back_keep(v):
    return (v, None)

def back_low(kept, grad):
    return (low(grad),)
low.defvjp(low_keep, low_pass)
low_back.defvjp(back_keep, back_low)
EPSILON = 1e-05
HIGH = lax.Precision.HIGHEST

def layer_norm(values, gain_vec, shift_vec):
    center = values - lax.optimization_barrier(jnp.mean(values, axis=-1, keepdims=True))
    inv_scale = lax.rsqrt(lax.optimization_barrier(jnp.mean(center * center, axis=-1, keepdims=True)) + EPSILON)
    return center * inv_scale * gain_vec + shift_vec

def rotary_tables(seq_length, head_size):
    half_size = head_size // 2
    inverse = jnp.exp(-jnp.log(10000.0) * jnp.arange(half_size, dtype=jnp.float32) * 2.0 / head_size)
    angles = jnp.arange(seq_length, dtype=jnp.float32)[:, None] * inverse[None, :]
    return (jnp.cos(angles), jnp.sin(angles))

def rotate(values, cosine_table, sine_table):
    half_size = values.shape[-1] // 2
    front_half = values[..., :half_size]
    back_half = values[..., half_size:]
    cos_wide = cosine_table[:, None, :]
    sin_wide = sine_table[:, None, :]
    return jnp.concatenate([front_half * cos_wide - back_half * sin_wide, back_half * cos_wide + front_half * sin_wide], axis=-1)

def attend_block(query_block, key_heads, value_heads, key_mask):
    raw_scores = jnp.einsum('qhd,khd->hqk', query_block, key_heads, precision=HIGH, preferred_element_type=jnp.float32)
    scores = low_back(raw_scores) * query_block.shape[-1] ** (-0.5)
    scores = jnp.where(key_mask[None, None, :], scores, -1e+30)
    highest = lax.optimization_barrier(jnp.max(scores, axis=-1, keepdims=True))
    exponent = jnp.exp(scores - highest)
    probability = exponent / lax.optimization_barrier(jnp.sum(exponent, axis=-1, keepdims=True))
    return jnp.einsum('hqk,khd->qhd', low(probability), value_heads, precision=HIGH, preferred_element_type=jnp.float32)

def layer(params, tokens, key_mask, cosine_table, sine_table):
    first_gain, first_bias, qkv_weight, qkv_bias, out_weight, out_bias, second_gain, second_bias, up_weight, up_bias, down_weight, down_bias = params
    seq_length, model_width = tokens.shape
    head_size = model_width // HEADS
    normed = low(layer_norm(tokens, first_gain, first_bias))
    projected = low_back(jnp.dot(normed, qkv_weight, precision=HIGH, preferred_element_type=jnp.float32)) + qkv_bias
    queries = low(rotate(projected[:, :model_width].reshape(seq_length, HEADS, head_size), cosine_table, sine_table))
    key_heads = low(rotate(projected[:, model_width:2 * model_width].reshape(seq_length, HEADS, head_size), cosine_table, sine_table))
    value_heads = low(projected[:, 2 * model_width:].reshape(seq_length, HEADS, head_size))
    block_rows = min(512, seq_length)
    query_blocks = queries.reshape(seq_length // block_rows, block_rows, HEADS, head_size)
    attend = jax.checkpoint(attend_block)
    attended = lax.map(lambda query_block: attend(query_block, key_heads, value_heads, key_mask), query_blocks)
    attended = low(low_back(attended.reshape(seq_length, model_width)))
    middle = tokens + low_back(jnp.dot(attended, out_weight, precision=HIGH, preferred_element_type=jnp.float32)) + out_bias
    second_normed = low(layer_norm(middle, second_gain, second_bias))
    pre_active = low_back(jnp.dot(second_normed, up_weight, precision=HIGH, preferred_element_type=jnp.float32)) + up_bias
    active = low(jax.nn.gelu(pre_active, approximate=False))
    return middle + low_back(jnp.dot(active, down_weight, precision=HIGH, preferred_element_type=jnp.float32)) + down_bias

def reference(tokens, lengths, first_gain, first_bias, qkv_weight, qkv_bias, out_weight, out_bias, second_gain, second_bias, up_weight, up_bias, down_weight, down_bias, cotangent):
    params = tuple((entry.astype(jnp.float32) for entry in (first_gain, first_bias, qkv_weight, qkv_bias, out_weight, out_bias, second_gain, second_bias, up_weight, up_bias, down_weight, down_bias)))
    seq_length = tokens.shape[1]
    cosine_table, sine_table = rotary_tables(seq_length, tokens.shape[2] // HEADS)
    positions = jnp.arange(seq_length, dtype=jnp.int32)

    def one_sequence(totals, entries):
        sequence, seq_size, grad_out = entries
        key_mask = positions < seq_size

        def forward(param_tuple, inputs):
            return layer(param_tuple, inputs, key_mask, cosine_table, sine_table)
        result, pullback = jax.vjp(forward, params, sequence.astype(jnp.float32))
        weighted = grad_out.astype(jnp.float32) * key_mask[:, None].astype(jnp.float32)
        param_grads, grad_input = pullback(weighted)
        totals = tuple((left_term + right_term for left_term, right_term in zip(totals, param_grads)))
        return (totals, (result.astype(jnp.bfloat16), grad_input.astype(jnp.bfloat16)))
    zero_grads = tuple((jnp.zeros_like(entry) for entry in params))
    totals, outputs = lax.scan(one_sequence, zero_grads, (tokens, lengths, cotangent))
    return (outputs[0], outputs[1], totals[0], totals[1], totals[2], totals[3], totals[4], totals[5], totals[6], totals[7], totals[8], totals[9], totals[10], totals[11])
```

```python
import functools

import jax
import jax.numpy as jnp
from jax import lax
from jax.experimental import pallas as pl
from jax.experimental.pallas import tpu as pltpu
from jax.sharding import PartitionSpec as P

HEADS = 12
EPSILON = 1e-05
F32 = jnp.float32
B16 = jnp.bfloat16
VMEM_LIMIT = 60 * 1024 * 1024


def params(steps=1, **more):
    return pltpu.CompilerParams(
        dimension_semantics=("arbitrary",) * steps, vmem_limit_bytes=VMEM_LIMIT, **more
    )


def dot_nt(a, b):
    return lax.dot_general(a, b, (((1,), (1,)), ((), ())), preferred_element_type=F32)


def dot_tn(a, b):
    return lax.dot_general(a, b, (((0,), (0,)), ((), ())), preferred_element_type=F32)


def rotary_tables(seq_length, head_size):
    half_size = head_size // 2
    inverse = jnp.exp(
        -jnp.log(10000.0) * jnp.arange(half_size, dtype=F32) * 2.0 / head_size
    )
    angles = jnp.arange(seq_length, dtype=F32)[:, None] * inverse[None, :]
    cosine, sine = jnp.cos(angles), jnp.sin(angles)
    return (
        jnp.concatenate([cosine] * 4, axis=1),
        jnp.concatenate([-sine, sine] * 2, axis=1),
    )


def spin(values, cosine, sine):
    lane = lax.broadcasted_iota(jnp.int32, values.shape, 1)
    partner = jnp.where(
        lane % 64 < 32, pltpu.roll(values, 96, 1), pltpu.roll(values, 32, 1)
    )
    return values * cosine + partner * sine


def qkv_kernel(blocks, x_ref, g_ref, b_ref, w_ref, wb_ref, c_ref, s_ref, a_ref, o_ref):
    step = pl.program_id(0)

    @pl.when(step == 0)
    def _():
        x = x_ref[...].astype(F32)
        center = x - jnp.mean(x, axis=-1, keepdims=True)
        scale = lax.rsqrt(jnp.mean(center * center, axis=-1, keepdims=True) + EPSILON)
        a_ref[...] = (center * scale * g_ref[...] + b_ref[...]).astype(B16)

    out = jnp.dot(a_ref[...], w_ref[...], preferred_element_type=F32) + wb_ref[...]

    @pl.when(step < 2 * blocks)
    def _():
        factor = jnp.where(step < blocks, 0.125, 1.0)
        for part in range(out.shape[1] // 128):
            lanes = slice(part * 128, part * 128 + 128)
            turned = spin(out[:, lanes], c_ref[...], s_ref[...])
            o_ref[:, lanes] = (turned * factor).astype(B16)

    @pl.when(step >= 2 * blocks)
    def _():
        o_ref[...] = out.astype(B16)


def qkv_call(x, gain, bias, weight, weight_bias, cosine, sine):
    rows, width = x.shape
    tile = 256
    blocks = width // tile
    return pl.pallas_call(
        functools.partial(qkv_kernel, blocks),
        grid=(3 * blocks,),
        in_specs=[
            pl.BlockSpec((rows, width), lambda j: (0, 0)),
            pl.BlockSpec((1, width), lambda j: (0, 0)),
            pl.BlockSpec((1, width), lambda j: (0, 0)),
            pl.BlockSpec((width, tile), lambda j: (0, j)),
            pl.BlockSpec((1, tile), lambda j: (0, j)),
            pl.BlockSpec((rows, 128), lambda j: (0, 0)),
            pl.BlockSpec((rows, 128), lambda j: (0, 0)),
        ],
        out_specs=[
            pl.BlockSpec((rows, width), lambda j: (0, 0)),
            pl.BlockSpec((rows, tile), lambda j: (0, j)),
        ],
        out_shape=[
            jax.ShapeDtypeStruct((rows, width), B16),
            jax.ShapeDtypeStruct((rows, 3 * width), B16),
        ],
        compiler_params=params(),
        cost_estimate=pl.CostEstimate(
            flops=2 * rows * width * 3 * width,
            bytes_accessed=2 * (2 * rows * width + 3 * width * width + 3 * rows * width),
            transcendentals=0,
        ),
        name="qkv",
    )(x, gain, bias, weight, weight_bias, cosine, sine)


def head_of(values, head):
    lane = lax.broadcasted_iota(jnp.int32, values.shape, 1)
    return jnp.where(lane // 64 == head, values, jnp.zeros_like(values))


QUERY_ROWS = 256


def attend_kernel(n_ref, q_ref, k_ref, v_ref, o_ref, l_ref):
    rows = q_ref.shape[0]

    def run(keys):
        k, v = k_ref[:keys, :], v_ref[:keys, :]
        for at in range(0, rows, QUERY_ROWS):
            q = q_ref[at : at + QUERY_ROWS, :]
            halves = []
            for head in range(2):
                scores = dot_nt(head_of(k, head), q)
                top = jnp.max(scores, axis=0, keepdims=True)
                weight = jnp.exp(scores - top)
                total = jnp.sum(weight, axis=0, keepdims=True)
                mixed = dot_tn(v, weight.astype(B16)) / total
                halves.append(mixed[head * 64 : head * 64 + 64, :])
                l_ref[0, head : head + 1, at : at + QUERY_ROWS] = top + jnp.log(total)
            o_ref[at : at + QUERY_ROWS, :] = jnp.concatenate(halves, axis=0).T.astype(B16)

    full = n_ref[0] == rows
    pl.when(full)(lambda: run(rows))
    pl.when(jnp.logical_not(full))(lambda: run(rows // 2))


def attend_call(lengths, packed):
    rows, width = packed.shape[0], packed.shape[1] // 3
    pairs = width // 128
    return pl.pallas_call(
        attend_kernel,
        grid_spec=pltpu.PrefetchScalarGridSpec(
            num_scalar_prefetch=1,
            grid=(pairs,),
            in_specs=[
                pl.BlockSpec((rows, 128), lambda j, n: (0, j)),
                pl.BlockSpec((rows, 128), lambda j, n: (0, pairs + j)),
                pl.BlockSpec((rows, 128), lambda j, n: (0, 2 * pairs + j)),
            ],
            out_specs=[
                pl.BlockSpec((rows, 128), lambda j, n: (0, j)),
                pl.BlockSpec((1, 2, rows), lambda j, n: (j, 0, 0)),
            ],
        ),
        out_shape=[
            jax.ShapeDtypeStruct((rows, width), B16),
            jax.ShapeDtypeStruct((pairs, 2, rows), F32),
        ],
        compiler_params=params(),
        cost_estimate=pl.CostEstimate(
            flops=16 * rows * rows * width,
            bytes_accessed=8 * rows * width,
            transcendentals=rows * rows * width // 64,
        ),
        name="attend",
    )(lengths, packed, packed, packed)


def attend_back_kernel(
    n_ref, q_ref, k_ref, v_ref, g_ref, l_ref, c_ref, s_ref, dq_ref, dk_ref, dv_ref, db_ref,
    dk_sum, dv_sum,
):
    rows = q_ref.shape[0]

    def run(keys):
        k, v = k_ref[:keys, :], v_ref[:keys, :]
        dk_sum[...] = jnp.zeros_like(dk_sum)
        dv_sum[...] = jnp.zeros_like(dv_sum)
        bias = jnp.zeros((1, 128), F32)
        for at in range(0, keys, QUERY_ROWS):
            span = slice(at, at + QUERY_ROWS)
            q, g = q_ref[span, :], g_ref[span, :]
            turned = None
            for head in range(2):
                k_head = head_of(k, head)
                weight = jnp.exp(dot_nt(k_head, q) - l_ref[0, head : head + 1, span])
                slope = dot_nt(head_of(v, head), g)
                inner = jnp.sum(weight * slope, axis=0, keepdims=True)
                change = (weight * (slope - inner)).astype(B16)
                dk_sum[:keys, :] += jnp.dot(
                    change, head_of(q, head), preferred_element_type=F32
                )
                dv_sum[:keys, :] += jnp.dot(
                    weight.astype(B16), head_of(g, head), preferred_element_type=F32
                )
                part = dot_tn(k_head, change)
                turned = part if turned is None else turned + part
            grad = spin(turned.T * 0.125, c_ref[span, :], -s_ref[span, :])
            bias = bias + jnp.sum(grad, axis=0, keepdims=True)
            dq_ref[span, :] = grad.astype(B16)
        if keys < rows:
            dq_ref[keys:, :] = jnp.zeros((rows - keys, 128), B16)
        dk = spin(dk_sum[...], c_ref[...], -s_ref[...])
        dk_ref[...] = dk.astype(B16)
        dv_ref[...] = dv_sum[...].astype(B16)
        db_ref[0, 0:1, :] = bias
        db_ref[0, 1:2, :] = jnp.sum(dk, axis=0, keepdims=True)
        db_ref[0, 2:3, :] = jnp.sum(dv_sum[...], axis=0, keepdims=True)

    full = n_ref[0] == rows
    pl.when(full)(lambda: run(rows))
    pl.when(jnp.logical_not(full))(lambda: run(rows // 2))


def attend_back_call(lengths, packed, grad, log_sums, cosine, sine):
    rows, width = grad.shape
    pairs = width // 128
    column = pl.BlockSpec((rows, 128), lambda j, n: (0, j))
    return pl.pallas_call(
        attend_back_kernel,
        grid_spec=pltpu.PrefetchScalarGridSpec(
            num_scalar_prefetch=1,
            grid=(pairs,),
            in_specs=[
                column,
                pl.BlockSpec((rows, 128), lambda j, n: (0, pairs + j)),
                pl.BlockSpec((rows, 128), lambda j, n: (0, 2 * pairs + j)),
                column,
                pl.BlockSpec((1, 2, rows), lambda j, n: (j, 0, 0)),
                pl.BlockSpec((rows, 128), lambda j, n: (0, 0)),
                pl.BlockSpec((rows, 128), lambda j, n: (0, 0)),
            ],
            out_specs=[
                column,
                column,
                column,
                pl.BlockSpec((1, 3, 128), lambda j, n: (j, 0, 0)),
            ],
            scratch_shapes=[pltpu.VMEM((rows, 128), F32), pltpu.VMEM((rows, 128), F32)],
        ),
        out_shape=[jax.ShapeDtypeStruct((rows, width), B16)] * 3
        + [jax.ShapeDtypeStruct((pairs, 3, 128), F32)],
        compiler_params=params(),
        cost_estimate=pl.CostEstimate(
            flops=40 * rows * rows * width,
            bytes_accessed=14 * rows * width,
            transcendentals=rows * rows * width // 64,
        ),
        name="attend_back",
    )(lengths, packed, packed, packed, grad, log_sums, cosine, sine)


def norm_parts(values):
    center = values - jnp.mean(values, axis=-1, keepdims=True)
    inverse = lax.rsqrt(jnp.mean(center * center, axis=-1, keepdims=True) + EPSILON)
    return center * inverse, inverse


def norm_back(grad, unit, inverse, gain):
    scaled = grad * gain
    return inverse * (
        scaled
        - jnp.mean(scaled, axis=-1, keepdims=True)
        - unit * jnp.mean(scaled * unit, axis=-1, keepdims=True)
    )


def gather_rows(shard):
    half = shard.shape[1] // 2
    mine = lax.dynamic_slice_in_dim(shard, lax.axis_index("dp") * half, half, axis=1)
    both = lax.all_gather(mine, ("fsdp", "dp"), axis=0, tiled=False)
    ranks, rows = both.shape[0] // 2, both.shape[1]
    both = both.reshape(ranks, 2, rows, half)
    return jnp.moveaxis(both, 1, 2).reshape(ranks * rows, 2 * half)


def scatter_rows(grad, ranks):
    rows, half = grad.shape[0] // ranks, grad.shape[1] // 2
    split = jnp.moveaxis(grad.astype(B16).reshape(ranks, rows, 2, half), 2, 1)
    mine = lax.psum_scatter(
        split.reshape(ranks * 2, rows, half), ("fsdp", "dp"), scatter_dimension=0, tiled=True
    )[0]
    both = lax.all_gather(mine, "dp", axis=0, tiled=False)
    return jnp.moveaxis(both, 0, 1).reshape(rows, 2 * half).astype(F32)


def local(
    ranks,
    tokens,
    lengths,
    first_gain,
    first_bias,
    qkv_weight,
    qkv_bias,
    out_weight,
    out_bias,
    second_gain,
    second_bias,
    up_weight,
    up_bias,
    down_weight,
    down_bias,
    cotangent,
):
    seq_length, model_width = tokens.shape[1:]
    vectors = (
        first_gain, first_bias, qkv_bias, out_bias, second_gain, second_bias, up_bias, down_bias,
    )
    sizes = [v.shape[0] for v in vectors]
    small = lax.all_gather(jnp.concatenate(vectors), "fsdp", axis=0, tiled=False)
    full_vectors, at = [], 0
    for size in sizes:
        full_vectors.append(small[:, at : at + size].reshape(1, -1).astype(F32))
        at += size
    gain_one, shift_one, qkv_shift, out_shift, gain_two, shift_two, up_shift, down_shift = (
        full_vectors
    )
    qkv_full = gather_rows(qkv_weight)
    out_full = gather_rows(out_weight)
    up_full = gather_rows(up_weight)
    down_full = gather_rows(down_weight)
    cosine, sine = rotary_tables(seq_length, model_width // HEADS)

    x = tokens[0]
    a1, packed = qkv_call(x, gain_one, shift_one, qkv_full, qkv_shift, cosine, sine)
    attended, log_sums = attend_call(lengths, packed)

    middle = x.astype(F32) + jnp.dot(attended, out_full, preferred_element_type=F32) + out_shift
    unit_two, inverse_two = norm_parts(middle)
    a2 = (unit_two * gain_two + shift_two).astype(B16)
    pre = jnp.dot(a2, up_full, preferred_element_type=F32) + up_shift
    active, gelu_pull = jax.vjp(functools.partial(jax.nn.gelu, approximate=False), pre)
    active_low = active.astype(B16)
    block_output = (
        middle + jnp.dot(active_low, down_full, preferred_element_type=F32) + down_shift
    ).astype(B16)

    valid = (jnp.arange(seq_length, dtype=jnp.int32) < lengths[0]).astype(F32)[:, None]
    grad_result = cotangent[0].astype(F32) * valid
    grad_low = grad_result.astype(B16)
    down_weight_grad = dot_tn(active_low, grad_low)
    (grad_pre,) = gelu_pull(dot_nt(grad_low, down_full))
    grad_pre_low = grad_pre.astype(B16)
    up_weight_grad = dot_tn(a2, grad_pre_low)
    grad_second = dot_nt(grad_pre_low, up_full)
    grad_middle = grad_result + norm_back(grad_second, unit_two, inverse_two, gain_two)
    grad_middle_low = grad_middle.astype(B16)
    out_weight_grad = dot_tn(attended, grad_middle_low)
    grad_attended = dot_nt(grad_middle_low, out_full).astype(B16)
    dq, dk, dv, mixed_sums = attend_back_call(
        lengths, packed, grad_attended, log_sums, cosine, sine
    )
    grad_mixed = jnp.concatenate([dq, dk, dv], axis=1)
    qkv_weight_grad = dot_tn(a1, grad_mixed)
    grad_normed = dot_nt(grad_mixed, qkv_full)
    unit_one, inverse_one = norm_parts(x.astype(F32))
    input_grad = (grad_middle + norm_back(grad_normed, unit_one, inverse_one, gain_one)).astype(B16)

    sums = (
        jnp.sum(grad_normed * unit_one, axis=0),
        jnp.sum(grad_normed, axis=0),
        jnp.moveaxis(mixed_sums, 1, 0).reshape(-1),
        jnp.sum(grad_middle, axis=0),
        jnp.sum(grad_second * unit_two, axis=0),
        jnp.sum(grad_second, axis=0),
        jnp.sum(grad_pre, axis=0),
        jnp.sum(grad_result, axis=0),
    )
    small_sums = jnp.concatenate([s.reshape(ranks, -1) for s in sums], axis=1)
    small_sums = lax.psum(
        lax.psum_scatter(small_sums, "fsdp", scatter_dimension=0, tiled=True)[0], "dp"
    )
    kept, at = [], 0
    for size in sizes:
        kept.append(small_sums[at : at + size])
        at += size
    return (
        block_output[None],
        input_grad[None],
        kept[0],
        kept[1],
        scatter_rows(qkv_weight_grad, ranks),
        kept[2],
        scatter_rows(out_weight_grad, ranks),
        kept[3],
        kept[4],
        kept[5],
        scatter_rows(up_weight_grad, ranks),
        kept[6],
        scatter_rows(down_weight_grad, ranks),
        kept[7],
    )


def solution(mesh):
    matrix, vector, rows = P("fsdp", None), P("fsdp"), P(("fsdp", "dp"), None, None)
    weights = (
        vector, vector, matrix, vector, matrix, vector,
        vector, vector, matrix, vector, matrix, vector,
    )
    return jax.shard_map(
        functools.partial(local, mesh.shape["fsdp"]),
        mesh=mesh,
        in_specs=(rows, P(("fsdp", "dp"))) + weights + (rows,),
        out_specs=(rows, rows) + weights,
        check_vma=False,
    )
```

```python
import functools

import jax
import jax.numpy as jnp
from jax import lax
from jax.experimental import pallas as pl
from jax.experimental.pallas import tpu as pltpu
from jax.sharding import PartitionSpec as P

HEADS = 12
EPSILON = 1e-05
F32 = jnp.float32
B16 = jnp.bfloat16
VMEM_LIMIT = 60 * 1024 * 1024


def params(steps=1, **more):
    return pltpu.CompilerParams(
        dimension_semantics=("arbitrary",) * steps, vmem_limit_bytes=VMEM_LIMIT, **more
    )


def dot_nt(a, b):
    return lax.dot_general(a, b, (((1,), (1,)), ((), ())), preferred_element_type=F32)


def dot_tn(a, b):
    return lax.dot_general(a, b, (((0,), (0,)), ((), ())), preferred_element_type=F32)


def rotary_tables(seq_length, head_size):
    half_size = head_size // 2
    inverse = jnp.exp(
        -jnp.log(10000.0) * jnp.arange(half_size, dtype=F32) * 2.0 / head_size
    )
    angles = jnp.arange(seq_length, dtype=F32)[:, None] * inverse[None, :]
    cosine, sine = jnp.cos(angles), jnp.sin(angles)
    return (
        jnp.concatenate([cosine] * 4, axis=1),
        jnp.concatenate([-sine, sine] * 2, axis=1),
    )


def spin(values, cosine, sine):
    lane = lax.broadcasted_iota(jnp.int32, values.shape, 1)
    partner = jnp.where(
        lane % 64 < 32, pltpu.roll(values, 96, 1), pltpu.roll(values, 32, 1)
    )
    return values * cosine + partner * sine


def qkv_kernel(blocks, x_ref, g_ref, b_ref, w_ref, wb_ref, c_ref, s_ref, a_ref, o_ref):
    step = pl.program_id(0)

    @pl.when(step == 0)
    def _():
        x = x_ref[...].astype(F32)
        center = x - jnp.mean(x, axis=-1, keepdims=True)
        scale = lax.rsqrt(jnp.mean(center * center, axis=-1, keepdims=True) + EPSILON)
        a_ref[...] = (center * scale * g_ref[...] + b_ref[...]).astype(B16)

    out = jnp.dot(a_ref[...], w_ref[...], preferred_element_type=F32) + wb_ref[...]

    @pl.when(step < 2 * blocks)
    def _():
        factor = jnp.where(step < blocks, 0.125, 1.0)
        for part in range(out.shape[1] // 128):
            lanes = slice(part * 128, part * 128 + 128)
            turned = spin(out[:, lanes], c_ref[...], s_ref[...])
            o_ref[:, lanes] = (turned * factor).astype(B16)

    @pl.when(step >= 2 * blocks)
    def _():
        o_ref[...] = out.astype(B16)


def qkv_call(x, gain, bias, weight, weight_bias, cosine, sine):
    rows, width = x.shape
    tile = 256
    blocks = width // tile
    return pl.pallas_call(
        functools.partial(qkv_kernel, blocks),
        grid=(3 * blocks,),
        in_specs=[
            pl.BlockSpec((rows, width), lambda j: (0, 0)),
            pl.BlockSpec((1, width), lambda j: (0, 0)),
            pl.BlockSpec((1, width), lambda j: (0, 0)),
            pl.BlockSpec((width, tile), lambda j: (0, j)),
            pl.BlockSpec((1, tile), lambda j: (0, j)),
            pl.BlockSpec((rows, 128), lambda j: (0, 0)),
            pl.BlockSpec((rows, 128), lambda j: (0, 0)),
        ],
        out_specs=[
            pl.BlockSpec((rows, width), lambda j: (0, 0)),
            pl.BlockSpec((rows, tile), lambda j: (0, j)),
        ],
        out_shape=[
            jax.ShapeDtypeStruct((rows, width), B16),
            jax.ShapeDtypeStruct((rows, 3 * width), B16),
        ],
        compiler_params=params(),
        cost_estimate=pl.CostEstimate(
            flops=2 * rows * width * 3 * width,
            bytes_accessed=2 * (2 * rows * width + 3 * width * width + 3 * rows * width),
            transcendentals=0,
        ),
        name="qkv",
    )(x, gain, bias, weight, weight_bias, cosine, sine)


def head_of(values, head):
    lane = lax.broadcasted_iota(jnp.int32, values.shape, 1)
    return jnp.where(lane // 64 == head, values, jnp.zeros_like(values))


QUERY_ROWS = 256
CHUNKS = 3


def attend_kernel(n_ref, q_ref, k_ref, v_ref, o_ref, l_ref):
    rows = q_ref.shape[0]

    def run(keys):
        k, v = k_ref[:keys, :], v_ref[:keys, :]
        for at in range(0, rows, QUERY_ROWS):
            q = q_ref[at : at + QUERY_ROWS, :]
            halves = []
            for head in range(2):
                scores = dot_nt(head_of(k, head), q)
                top = jnp.max(scores, axis=0, keepdims=True)
                weight = jnp.exp(scores - top)
                total = jnp.sum(weight, axis=0, keepdims=True)
                mixed = dot_tn(v, weight.astype(B16)) / total
                halves.append(mixed[head * 64 : head * 64 + 64, :])
                l_ref[0, head : head + 1, at : at + QUERY_ROWS] = top + jnp.log(total)
            o_ref[at : at + QUERY_ROWS, :] = jnp.concatenate(halves, axis=0).T.astype(B16)

    full = n_ref[0] == rows
    pl.when(full)(lambda: run(rows))
    pl.when(jnp.logical_not(full))(lambda: run(rows // 2))


def attend_call(lengths, packed, start, count):
    rows, pairs = packed.shape[0], packed.shape[1] // 384
    width = count * 128
    return pl.pallas_call(
        attend_kernel,
        grid_spec=pltpu.PrefetchScalarGridSpec(
            num_scalar_prefetch=1,
            grid=(count,),
            in_specs=[
                pl.BlockSpec((rows, 128), lambda j, n: (0, start + j)),
                pl.BlockSpec((rows, 128), lambda j, n: (0, pairs + start + j)),
                pl.BlockSpec((rows, 128), lambda j, n: (0, 2 * pairs + start + j)),
            ],
            out_specs=[
                pl.BlockSpec((rows, 128), lambda j, n: (0, j)),
                pl.BlockSpec((1, 2, rows), lambda j, n: (j, 0, 0)),
            ],
        ),
        out_shape=[
            jax.ShapeDtypeStruct((rows, width), B16),
            jax.ShapeDtypeStruct((count, 2, rows), F32),
        ],
        compiler_params=params(),
        cost_estimate=pl.CostEstimate(
            flops=16 * rows * rows * width,
            bytes_accessed=8 * rows * width,
            transcendentals=rows * rows * width // 64,
        ),
        name="attend",
    )(lengths, packed, packed, packed)


def attend_back_kernel(
    n_ref, q_ref, k_ref, v_ref, g_ref, l_ref, c_ref, s_ref, dq_ref, dk_ref, dv_ref, db_ref,
    dk_sum, dv_sum,
):
    rows = q_ref.shape[0]

    def run(keys):
        k, v = k_ref[:keys, :], v_ref[:keys, :]
        dk_sum[...] = jnp.zeros_like(dk_sum)
        dv_sum[...] = jnp.zeros_like(dv_sum)
        bias = jnp.zeros((1, 128), F32)
        for at in range(0, keys, QUERY_ROWS):
            span = slice(at, at + QUERY_ROWS)
            q, g = q_ref[span, :], g_ref[span, :]
            turned = None
            for head in range(2):
                k_head = head_of(k, head)
                weight = jnp.exp(dot_nt(k_head, q) - l_ref[0, head : head + 1, span])
                slope = dot_nt(head_of(v, head), g)
                inner = jnp.sum(weight * slope, axis=0, keepdims=True)
                change = (weight * (slope - inner)).astype(B16)
                dk_sum[:keys, :] += jnp.dot(
                    change, head_of(q, head), preferred_element_type=F32
                )
                dv_sum[:keys, :] += jnp.dot(
                    weight.astype(B16), head_of(g, head), preferred_element_type=F32
                )
                part = dot_tn(k_head, change)
                turned = part if turned is None else turned + part
            grad = spin(turned.T * 0.125, c_ref[span, :], -s_ref[span, :])
            bias = bias + jnp.sum(grad, axis=0, keepdims=True)
            dq_ref[span, :] = grad.astype(B16)
        if keys < rows:
            dq_ref[keys:, :] = jnp.zeros((rows - keys, 128), B16)
        dk = spin(dk_sum[...], c_ref[...], -s_ref[...])
        dk_ref[...] = dk.astype(B16)
        dv_ref[...] = dv_sum[...].astype(B16)
        db_ref[0, 0:1, :] = bias
        db_ref[0, 1:2, :] = jnp.sum(dk, axis=0, keepdims=True)
        db_ref[0, 2:3, :] = jnp.sum(dv_sum[...], axis=0, keepdims=True)

    full = n_ref[0] == rows
    pl.when(full)(lambda: run(rows))
    pl.when(jnp.logical_not(full))(lambda: run(rows // 2))


def attend_back_call(lengths, packed, grad, log_sums, cosine, sine, start):
    rows, pairs = grad.shape[0], packed.shape[1] // 384
    count = log_sums.shape[0]
    width = count * 128
    column = pl.BlockSpec((rows, 128), lambda j, n: (0, j))
    return pl.pallas_call(
        attend_back_kernel,
        grid_spec=pltpu.PrefetchScalarGridSpec(
            num_scalar_prefetch=1,
            grid=(count,),
            in_specs=[
                pl.BlockSpec((rows, 128), lambda j, n: (0, start + j)),
                pl.BlockSpec((rows, 128), lambda j, n: (0, pairs + start + j)),
                pl.BlockSpec((rows, 128), lambda j, n: (0, 2 * pairs + start + j)),
                pl.BlockSpec((rows, 128), lambda j, n: (0, start + j)),
                pl.BlockSpec((1, 2, rows), lambda j, n: (j, 0, 0)),
                pl.BlockSpec((rows, 128), lambda j, n: (0, 0)),
                pl.BlockSpec((rows, 128), lambda j, n: (0, 0)),
            ],
            out_specs=[
                column,
                column,
                column,
                pl.BlockSpec((1, 3, 128), lambda j, n: (j, 0, 0)),
            ],
            scratch_shapes=[pltpu.VMEM((rows, 128), F32), pltpu.VMEM((rows, 128), F32)],
        ),
        out_shape=[jax.ShapeDtypeStruct((rows, width), B16)] * 3
        + [jax.ShapeDtypeStruct((count, 3, 128), F32)],
        compiler_params=params(),
        cost_estimate=pl.CostEstimate(
            flops=40 * rows * rows * width,
            bytes_accessed=14 * rows * width,
            transcendentals=rows * rows * width // 64,
        ),
        name="attend_back",
    )(lengths, packed, packed, packed, grad, log_sums, cosine, sine)


def norm_parts(values):
    center = values - jnp.mean(values, axis=-1, keepdims=True)
    inverse = lax.rsqrt(jnp.mean(center * center, axis=-1, keepdims=True) + EPSILON)
    return center * inverse, inverse


def norm_back(grad, unit, inverse, gain):
    scaled = grad * gain
    return inverse * (
        scaled
        - jnp.mean(scaled, axis=-1, keepdims=True)
        - unit * jnp.mean(scaled * unit, axis=-1, keepdims=True)
    )


def grid_of(ranks):
    return {16: (4, 2, 2), 128: (4, 4, 8)}.get(ranks, (ranks,))


def along(sizes, dim, shift):
    stride = 1
    for size in sizes[dim + 1 :]:
        stride *= size
    ranks = stride
    for size in sizes[: dim + 1]:
        ranks *= size
    pairs = []
    for rank in range(ranks):
        place = rank // stride % sizes[dim]
        pairs.append((rank, rank + ((place + shift) % sizes[dim] - place) * stride))
    return pairs, lax.axis_index("fsdp") // stride % sizes[dim]


def swap(value):
    return lax.ppermute(value, "dp", [(0, 1), (1, 0)])


def gather_grid(value, sizes, order):
    value = value.reshape((1,) * len(sizes) + value.shape)
    for dim in order:
        size = sizes[dim]
        pieces, place = [value], None
        for shift in range(1, size):
            pairs, place = along(sizes, dim, shift)
            pieces.append(lax.ppermute(value, "fsdp", pairs))
        if size == 2:
            first = place == 0
            value = jnp.concatenate(
                [jnp.where(first, *pieces), jnp.where(first, *pieces[::-1])], axis=dim
            )
        else:
            shape = value.shape[:dim] + (size,) + value.shape[dim + 1 :]
            value = jnp.zeros(shape, value.dtype)
            for shift, piece in enumerate(pieces):
                value = lax.dynamic_update_slice_in_dim(
                    value, piece, (place + size - shift) % size, axis=dim
                )
    return value.reshape((-1,) + value.shape[len(sizes) :])


def scatter_grid(value, sizes, order):
    kind = value.dtype
    value = value.reshape(sizes + value.shape[1:])
    for dim in order:
        size = sizes[dim]
        total, place = None, None
        for shift in range(1, size):
            pairs, place = along(sizes, dim, shift)
            piece = lax.dynamic_slice_in_dim(value, (place + shift) % size, 1, axis=dim)
            piece = lax.ppermute(piece.astype(kind), "fsdp", pairs).astype(F32)
            total = piece if total is None else total + piece
        if total is not None:
            value = total + lax.dynamic_slice_in_dim(value, place, 1, axis=dim).astype(F32)
            if dim != order[-1]:
                value = value.astype(kind)
    return value.reshape(value.shape[len(sizes) :]).astype(F32)


def half_of(value, which):
    half = value.shape[-1] // 2
    return lax.dynamic_slice_in_dim(value, which * half, half, axis=value.ndim - 1)


def in_order(mine, other):
    first = lax.axis_index("dp") == 0
    return jnp.where(first, mine, other), jnp.where(first, other, mine)


def fold(grad):
    core = lax.axis_index("dp")
    taken = swap(half_of(grad, 1 - core))
    return (half_of(grad, core).astype(F32) + taken.astype(F32)).astype(B16)


def whole(mine):
    return jnp.concatenate(in_order(mine, swap(mine)), axis=-1)


def local(
    ranks,
    tokens,
    lengths,
    first_gain,
    first_bias,
    qkv_weight,
    qkv_bias,
    out_weight,
    out_bias,
    second_gain,
    second_bias,
    up_weight,
    up_bias,
    down_weight,
    down_bias,
    cotangent,
):
    seq_length, model_width = tokens.shape[1:]
    vectors = (
        first_gain, first_bias, qkv_bias, out_bias, second_gain, second_bias, up_bias, down_bias,
    )
    sizes = [v.shape[0] for v in vectors]
    grid = grid_of(ranks)
    forth = tuple(range(len(grid)))
    other = forth[:1] + forth[:0:-1]
    core = lax.axis_index("dp")
    small = gather_grid(jnp.concatenate(vectors)[None], grid, forth)[:, 0]
    full_vectors, at = [], 0
    for size in sizes:
        full_vectors.append(small[:, at : at + size].reshape(1, -1).astype(F32))
        at += size
    gain_one, shift_one, qkv_shift, out_shift, gain_two, shift_two, up_shift, down_shift = (
        full_vectors
    )
    qkv_half, out_half = half_of(qkv_weight, core), half_of(out_weight, core)
    cut = 2 * qkv_half.shape[1] // 3
    part_one = gather_grid(qkv_half[:, :cut], grid, forth)
    part_two = gather_grid(jnp.concatenate([qkv_half[:, cut:], out_half], axis=1), grid, other)
    up_half, down_half, part_one, part_two = lax.optimization_barrier(
        (half_of(up_weight, core), half_of(down_weight, core), part_one, part_two)
    )
    one_low, one_high = in_order(part_one, swap(part_one))
    two_low, two_high = in_order(part_two, swap(part_two))
    rest = qkv_half.shape[1] - cut
    qkv_full = jnp.concatenate(
        [one_low, two_low[..., :rest], one_high, two_high[..., :rest]], axis=-1
    ).reshape(model_width, -1)
    out_full = jnp.concatenate([two_low[..., rest:], two_high[..., rest:]], axis=-1).reshape(
        model_width, -1
    )
    up_full = whole(gather_grid(up_half, grid, forth)).reshape(model_width, -1)
    down_full = whole(gather_grid(down_half, grid, other)).reshape(-1, model_width)
    cosine, sine = rotary_tables(seq_length, model_width // HEADS)

    x = tokens[0]
    a1, packed = qkv_call(x, gain_one, shift_one, qkv_full, qkv_shift, cosine, sine)
    pairs = model_width // 128
    chunks = [(start, pairs // CHUNKS) for start in range(0, pairs, pairs // CHUNKS)]
    heads = [attend_call(lengths, packed, *chunk) for chunk in chunks]
    attended = jnp.concatenate([head[0] for head in heads], axis=1)

    middle = x.astype(F32) + jnp.dot(attended, out_full, preferred_element_type=F32) + out_shift
    unit_two, inverse_two = norm_parts(middle)
    a2 = (unit_two * gain_two + shift_two).astype(B16)
    pre = jnp.dot(a2, up_full, preferred_element_type=F32) + up_shift
    active, gelu_pull = jax.vjp(functools.partial(jax.nn.gelu, approximate=False), pre)
    active_low = active.astype(B16)
    block_output = (
        middle + jnp.dot(active_low, down_full, preferred_element_type=F32) + down_shift
    ).astype(B16)

    valid = (jnp.arange(seq_length, dtype=jnp.int32) < lengths[0]).astype(F32)[:, None]
    grad_result = cotangent[0].astype(F32) * valid
    grad_low = grad_result.astype(B16)
    down_weight_grad = dot_tn(active_low, grad_low).astype(B16)
    (grad_pre,) = gelu_pull(dot_nt(grad_low, down_full))
    grad_pre_low = grad_pre.astype(B16)
    up_weight_grad = dot_tn(a2, grad_pre_low).astype(B16)
    grad_second = dot_nt(grad_pre_low, up_full)
    grad_middle = grad_result + norm_back(grad_second, unit_two, inverse_two, gain_two)
    grad_middle_low = grad_middle.astype(B16)
    out_weight_grad = dot_tn(attended, grad_middle_low).astype(B16)
    grad_attended = dot_nt(grad_middle_low, out_full).astype(B16)
    grad_attended, down_weight_grad, up_weight_grad = lax.optimization_barrier(
        (grad_attended, down_weight_grad, up_weight_grad)
    )
    backs = [
        attend_back_call(lengths, packed, grad_attended, head[1], cosine, sine, chunk[0])
        for head, chunk in zip(heads, chunks)
    ]
    grad_mixed = jnp.concatenate([back[i] for i in range(3) for back in backs], axis=1)
    mixed_sums = jnp.concatenate([back[3] for back in backs], axis=0)
    qkv_weight_grad = dot_tn(a1, grad_mixed).astype(B16)
    grad_normed = dot_nt(grad_mixed, qkv_full)
    unit_one, inverse_one = norm_parts(x.astype(F32))
    input_grad = (grad_middle + norm_back(grad_normed, unit_one, inverse_one, gain_one)).astype(B16)

    sums = (
        jnp.sum(grad_normed * unit_one, axis=0),
        jnp.sum(grad_normed, axis=0),
        jnp.moveaxis(mixed_sums, 1, 0).reshape(-1),
        jnp.sum(grad_middle, axis=0),
        jnp.sum(grad_second * unit_two, axis=0),
        jnp.sum(grad_second, axis=0),
        jnp.sum(grad_pre, axis=0),
        jnp.sum(grad_result, axis=0),
    )
    small_sums = jnp.concatenate([s.reshape(ranks, -1) for s in sums], axis=1)
    small_sums = small_sums + swap(small_sums)
    back, back_other = forth[::-1], other[::-1]
    small_sums = scatter_grid(small_sums[:, None], grid, back)[0]

    def by_rank(grad):
        return fold(grad).reshape(ranks, grad.shape[0] // ranks, -1)

    up_sum = whole(scatter_grid(by_rank(up_weight_grad), grid, back))
    down_sum = whole(scatter_grid(by_rank(down_weight_grad), grid, back_other))
    qkv_rank, out_rank = by_rank(qkv_weight_grad), by_rank(out_weight_grad)
    one_sum = scatter_grid(qkv_rank[..., :cut], grid, back)
    two_sum = scatter_grid(
        jnp.concatenate([qkv_rank[..., cut:], out_rank], axis=-1), grid, back_other
    )
    qkv_sum = whole(jnp.concatenate([one_sum, two_sum[:, :rest]], axis=1))
    out_sum = whole(two_sum[:, rest:])
    kept, at = [], 0
    for size in sizes:
        kept.append(small_sums[at : at + size])
        at += size
    return (
        block_output[None],
        input_grad[None],
        kept[0],
        kept[1],
        qkv_sum,
        kept[2],
        out_sum,
        kept[3],
        kept[4],
        kept[5],
        up_sum,
        kept[6],
        down_sum,
        kept[7],
    )


def solution(mesh):
    matrix, vector, rows = P("fsdp", None), P("fsdp"), P(("fsdp", "dp"), None, None)
    weights = (
        vector, vector, matrix, vector, matrix, vector,
        vector, vector, matrix, vector, matrix, vector,
    )
    return jax.shard_map(
        functools.partial(local, mesh.shape["fsdp"]),
        mesh=mesh,
        in_specs=(rows, P(("fsdp", "dp"))) + weights + (rows,),
        out_specs=(rows, rows) + weights,
        check_vma=False,
    )
```
